32 devices in a mesh: vol: 8 (over z, y), pix: 4 (over x, core).
Axes of the slice: x: 2, y: 2, z: 4, core: 2. Of those that a mesh axis runs over, the one named last changes fastest.
Arguments:
- kernel: bfloat16 [524288, 128], P(('vol', 'pix')), may hold values from 0 to 0.25
- pressure: bfloat16 [524288], P(('vol', 'pix')), may hold values from 0.049804688 to 2
- velocity: bfloat16 [524288], P(('vol', 'pix')), may hold values from -4 to 4
- entry_slot: int32 [32, 16384], P(('vol', 'pix')), may hold values from 0 to 1023, never falling along the last dimension, each value on 1 to 32 neighbouring positions
- slot_tile: int32 [32, 1024], P(('vol', 'pix')), may hold values from 0 to 8191, as said below
- tile_owner: int32 [8192], replicated, may hold values from 0 to 3, as said below
Outputs:
- owned_tiles: float32 [16384, 256], P(('vol', 'pix'))
- shell_map: float32 [8192, 256], P('vol')
The draws below stay inside these ranges and needn't reach their ends.
Inputs may be any that keep to these rules, and one draw needn't show every extreme that they name: `entry_slot`: for each device the slot numbers never fall along its 16384 crossings; every slot has at least one crossing and at most 32. `tile_owner`: within every block of 1024 consecutive tiles each pix index owns 256 // 2 to 512 tiles, and one owner of each block owns exactly 512. `slot_tile`: the 1024 tiles of one device are distinct; at most 64 of them belong to any one owning device (vol index t // 1024, pix index tile_owner[t]), and one owning device gets exactly 64 from every device.
All inputs are finite; a program needn't handle non-finite values.
Results may differ from the reference program's by a relative error of at most 0.0003.
Values sent between devices are 32-bit elements; how exact they have to be, the bound alone decides.
A program may use at most 64 MiB of HBM per device.

```python
import math
import jax
import jax.numpy as jnp
import numpy as np
from jax import lax

PIX_TILE = 128
CHANNELS = 2
ENTRIES = 16384
SLOTS = 1024
TILE_DEV = 256
TILE_V = 1024
TILES = 8192
OWN_MAX = 512
CAP = 64
N_VOL = 8
N_PIX = 4
DEVICES = 32


def ownership(key):
    groups = TILE_V // TILE_DEV
    vol_count = TILES // TILE_V
    least_owned = TILE_DEV // 2
    most_owned = 2 * TILE_DEV
    remainder = TILE_V - most_owned - (groups - 1) * least_owned
    labels = jnp.arange(groups, dtype=jnp.int32)

    def one_block(block_key):
        busiest_key, pool_key, mix_key = jax.random.split(block_key, 3)
        busiest = jax.random.randint(busiest_key, (), 0, groups, dtype=jnp.int32)
        baseline = jnp.repeat(labels, least_owned)
        extra_top = jnp.full((most_owned - least_owned,), 1, jnp.int32) * busiest
        token_pool = jax.random.permutation(pool_key, jnp.repeat(labels, most_owned - least_owned))
        ordering = jnp.argsort((token_pool == busiest).astype(jnp.int32), stable=True)
        chosen = token_pool[ordering][:remainder]
        block_owner = jnp.concatenate([baseline, extra_top, chosen]).astype(jnp.int32)
        return (jax.random.permutation(mix_key, block_owner), busiest)
    owners, busiest_overall = jax.vmap(one_block)(jax.random.split(key, vol_count))
    heavy_vol = jax.random.randint(jax.random.fold_in(key, 7), (), 0, vol_count, dtype=jnp.int32)
    heavy_device = heavy_vol * groups + busiest_overall[heavy_vol]
    return (owners.astype(jnp.int32), heavy_device.astype(jnp.int32))


def draw_tile_owner(key, part):
    owners, heavy_device = ownership(jax.random.fold_in(key, 101))
    return owners.reshape(TILES)


def draw_slot_tile(key, part):
    owners, heavy_device = ownership(jax.random.fold_in(key, 101))
    groups = TILE_V // TILE_DEV
    vol_count = TILES // TILE_V
    device_count = vol_count * groups
    flat_owner = owners.reshape(TILES)
    holder = jnp.arange(TILES, dtype=jnp.int32) // TILE_V * groups + flat_owner
    held_count = jax.ops.segment_sum(jnp.ones((TILES,), jnp.int32), holder, num_segments=device_count)
    first_row = (jnp.cumsum(held_count, dtype=jnp.int32) - held_count).astype(jnp.int32)
    labels = jnp.arange(device_count, dtype=jnp.int32)

    def one_device(device_key):
        pool_key, ranking_random_key, mix_key = jax.random.split(device_key, 3)
        token_pool = jax.random.permutation(pool_key, jnp.repeat(labels, CAP))
        ordering = jnp.argsort((token_pool == heavy_device).astype(jnp.int32), stable=True)
        chosen = token_pool[ordering][:SLOTS - CAP]
        wanted = jax.ops.segment_sum(jnp.ones((SLOTS - CAP,), jnp.int32), chosen, num_segments=device_count)
        wanted = wanted + CAP * (labels == heavy_device).astype(jnp.int32)
        shuffle = jax.random.permutation(ranking_random_key, TILES).astype(jnp.int32)
        grouped = jnp.argsort(holder * TILES + shuffle, stable=True).astype(jnp.int32)
        position = jnp.arange(TILES, dtype=jnp.int32) - first_row[holder[grouped]]
        selected = position < wanted[holder[grouped]]
        positions = jnp.nonzero(selected, size=SLOTS)[0]
        tile_ids = grouped[positions].astype(jnp.int32)
        return jax.random.permutation(mix_key, tile_ids)
    device_keys = jax.random.split(jax.random.fold_in(key, 202), device_count)
    return jax.vmap(one_device)(device_keys).astype(jnp.int32)


def levels(rng, dims, cuts, low, high):
    def one(axis_at, blocks):
        heights = jax.random.uniform(jax.random.fold_in(jax.random.fold_in(rng, 6), axis_at), (blocks,), jnp.float32, low / len(cuts), high / len(cuts))
        return jnp.repeat(jnp.exp(heights), dims[axis_at] // blocks).reshape((-1,) + (1,) * (len(dims) - axis_at - 1))

    factor_of = one(*cuts[0])
    for cut in cuts[1:]:
        factor_of = factor_of * one(*cut)
    return factor_of


def profile(number_of, total, limit, skew):
    loads = [(1 << 20) // math.isqrt(rank ** skew) + 1 for rank in range(2, number_of + 1)]
    spare, counts = total - limit - (number_of - 1), [1] * (number_of - 1)
    while spare > 0:
        candidates = [i for i in range(number_of - 1) if counts[i] < limit]
        pool, left = sum([loads[i] for i in candidates]), spare
        for i in candidates:
            more = min(limit - counts[i], max(1, left * loads[i] // pool), spare)
            counts[i] = counts[i] + more
            spare = spare - more
    return np.array([limit] + counts)


def ragged(stream_key, number_of, total, limit, slope):
    if number_of == 2:
        one = jax.random.randint(stream_key, (), max(1, total - limit), min(limit, total - 1) + 1)
        return jnp.stack([one, total - one])
    tallies = jnp.asarray(profile(number_of, total, limit, slope), jnp.int32)
    twos = (number_of - 1) // 2
    donor, receiver = tallies[1:1 + 2 * twos:2], tallies[2:2 + 2 * twos:2]
    margin = jnp.minimum(donor - 1, limit - receiver)
    passed = jax.random.randint(jax.random.fold_in(stream_key, 1), (twos,), 0, 1 << 20) % (margin + 1)
    tallies = tallies.at[1:1 + 2 * twos:2].set(donor - passed).at[2:2 + 2 * twos:2].set(receiver + passed)
    return tallies[jax.random.permutation(jax.random.fold_in(stream_key, 2), number_of)]


def normal_values(rng, shape, spread, reach, shards=(), kind=jnp.bfloat16):
    loudness = levels(rng, shape, shards, -0.22, 0.18) if shards else 1.0
    values = jax.random.normal(rng, shape, jnp.float32) * spread * loudness
    return jnp.minimum(jnp.maximum(values, -reach), reach).astype(kind)


def setup_inputs(seed: int = 0) -> dict:
    splits = jax.random.split(jax.random.key(seed), 7)
    return {
        "kernel": jnp.clip(0.25 * jax.random.uniform(splits[0], (DEVICES * ENTRIES, PIX_TILE), jnp.float32) ** levels(splits[0], (DEVICES * ENTRIES, PIX_TILE), ((0, 32),), -0.2, 0.2), 0.0, 0.25).astype(jnp.bfloat16),
        "pressure": jnp.clip(jnp.exp(math.log(2.0) - 3.6927934 * jax.random.uniform(splits[1], (DEVICES * ENTRIES,), jnp.float32) ** levels(splits[1], (DEVICES * ENTRIES,), ((0, 32),), -0.2, 0.2)), 0.049804688, 2.0).astype(jnp.bfloat16),
        "velocity": normal_values(splits[2], (DEVICES * ENTRIES,), 1.0, 4.0, ((0, 32),)),
        "entry_slot": jax.vmap(lambda own: jnp.searchsorted(jnp.cumsum(ragged(own, SLOTS, ENTRIES, 2 * ENTRIES // SLOTS, 1)), jnp.arange(ENTRIES), side="right"))(jax.random.split(splits[3], DEVICES)).reshape((DEVICES, ENTRIES)).astype(jnp.int32),
        "slot_tile": draw_slot_tile(jax.random.fold_in(splits[6], 71), 0),
        "tile_owner": draw_tile_owner(jax.random.fold_in(splits[6], 71), 0),
    }


def reference(kernel, pressure, velocity, entry_slot, slot_tile, tile_owner):
    kernel_weights = kernel.reshape(DEVICES, ENTRIES, PIX_TILE)
    amplitude = jnp.stack([pressure, velocity], axis=-1).reshape(DEVICES, ENTRIES, CHANNELS)

    def accumulate(running, inputs):
        device_kernel, device_amplitude, device_slot, device_tile = inputs
        pixel_products = device_amplitude.astype(jnp.float32)[:, :, None] * device_kernel.astype(jnp.float32)[:, None, :]
        partial_value = jax.ops.segment_sum(pixel_products.reshape(ENTRIES, CHANNELS * PIX_TILE), device_slot, num_segments=SLOTS)
        return running.at[device_tile].add(partial_value), None

    start_value = jnp.zeros((TILES, CHANNELS * PIX_TILE), jnp.float32)
    shell_map, unused = lax.scan(accumulate, start_value, (kernel_weights, amplitude, entry_slot, slot_tile))
    owners = tile_owner.reshape(N_VOL, TILE_V)
    matches = owners[:, None, :] == jnp.arange(N_PIX, dtype=jnp.int32)[None, :, None]
    owner_ranking = jnp.cumsum(matches.astype(jnp.int32), axis=2, dtype=jnp.int32) - 1
    owner_rank = jnp.sum(jnp.where(matches, owner_ranking, 0), axis=1, dtype=jnp.int32)
    vol_ids = jnp.arange(N_VOL, dtype=jnp.int32)[:, None]
    destination = ((vol_ids * N_PIX + owners) * OWN_MAX + owner_rank).astype(jnp.int32)
    owned_tiles = jnp.zeros((DEVICES * OWN_MAX, CHANNELS * PIX_TILE), jnp.float32)
    owned_tiles = owned_tiles.at[destination.reshape(TILES)].set(shell_map)
    return owned_tiles, shell_map
```

```python
import functools

import jax
import jax.numpy as jnp
from jax import lax
from jax.experimental import pallas as pl
from jax.experimental.pallas import tpu as pltpu
from jax.sharding import PartitionSpec as P

MESH = pl.DeviceIdType.MESH
LANES = 128
BLOCK = 256
WINDOW = 48
F32 = jnp.float32
BF16 = jnp.bfloat16
I32 = jnp.int32


def iota(shape, axis):
    return lax.broadcasted_iota(I32, shape, axis)


def onehot(mask):
    return jnp.where(mask, 1.0, 0.0).astype(BF16)


def dot(a, b):
    return jnp.dot(a, b, preferred_element_type=F32)


def halves(x):
    high = x.astype(BF16)
    low = (x - high.astype(F32)).astype(BF16)
    return jnp.concatenate([high, low], axis=1)


def prepare(
    dims, base_ref, last_ref, kern_hbm, thermal_ref, kinetic_ref, slot_ref, tile_ref, owner_ref,
    out_ref, ids_ref, code_ref, kern_ref, thermal32, kinetic32, part_ref, split_ref, sems,
):
    vol_count, pix_count, slots, block_tiles, owned_most, cap = dims
    device_count = vol_count * pix_count
    entries = kern_ref.shape[0]
    blocks = entries // BLOCK
    pieces = sems.shape[0]
    piece = entries // pieces

    def fetch(q):
        rows = pl.ds(q * piece, piece)
        return pltpu.make_async_copy(kern_hbm.at[rows], kern_ref.at[rows], sems.at[q])

    for q in range(pieces):
        fetch(q).start()

    high_count = owner_ref.shape[0]
    block_high = block_tiles // LANES
    owner = jnp.transpose(owner_ref[...].astype(F32))
    lower = onehot(iota((LANES, LANES), 1) < iota((LANES, LANES), 0))
    first, second = iota((high_count, high_count), 0), iota((high_count, high_count), 1)
    before = onehot((first < second) & (first // block_high == second // block_high))
    rank = jnp.zeros((LANES, high_count), F32)
    for p in range(pix_count):
        mine = owner == p
        ones = jnp.where(mine, 1.0, 0.0)
        inside = dot(lower, ones.astype(BF16))
        total = jnp.broadcast_to(jnp.sum(ones, axis=0, keepdims=True), (8, high_count))
        ahead = dot(total.astype(BF16), before)[0:1]
        rank = rank + jnp.where(mine, inside + ahead, 0.0)

    code = owner * owned_most + rank
    first_high = lax.axis_index("vol") * block_high
    lane = iota((LANES, high_count), 1)
    for h in range(block_high):
        column = jnp.sum(jnp.where(lane == first_high + h, code, 0.0), axis=1, keepdims=True)
        code_ref[h * LANES:(h + 1) * LANES, :] = jnp.broadcast_to(
            column, (LANES, LANES)
        ).astype(I32)

    parts = max(1, owned_most // 256)
    rank_high = jnp.floor(rank * (1.0 / 256.0))
    rank_low = rank - 256.0 * rank_high
    table = jnp.concatenate([owner * parts + rank_high, rank_low], axis=0).astype(BF16)
    tile = tile_ref[...]
    high, low = tile // LANES, tile % LANES
    found = dot(table, onehot(iota((high_count, slots), 0) == high))
    pick = iota((LANES, slots), 0) == low
    both = jnp.sum(jnp.where(pick, found[:LANES], 0.0), axis=0, keepdims=True).astype(I32)
    row_low = jnp.sum(jnp.where(pick, found[LANES:], 0.0), axis=0, keepdims=True)
    slot_owner = both // parts
    row_high = (both - slot_owner * parts).astype(F32)
    target = high // block_high * pix_count + slot_owner
    to_device = iota((device_count, slots), 0) == target
    ones = jnp.where(to_device, 1.0, 0.0)
    upper = onehot(iota((LANES, LANES), 0) < iota((LANES, LANES), 1))
    carry = jnp.zeros((device_count, 1), F32)
    position = []
    for j in range(slots // LANES):
        chunk = ones[:, j * LANES:(j + 1) * LANES]
        ranks = dot(chunk.astype(BF16), upper) + carry
        position.append(jnp.sum(chunk * ranks, axis=0, keepdims=True))
        carry = carry + jnp.sum(chunk, axis=1, keepdims=True)
    position = jnp.concatenate(position, axis=1).astype(I32)
    bucket = target * cap + position

    places = onehot(iota((LANES, slots), 0) % cap == position)
    values = jnp.concatenate(
        [jnp.where(to_device, row_high, 0.0), jnp.where(to_device, row_low + 1.0, 0.0)], axis=0
    )
    placed = lax.dot_general(
        values.astype(BF16), places, (((1,), (1,)), ((), ())), preferred_element_type=F32
    )
    rows = placed[:device_count] * 256.0 + placed[device_count:] - 1.0
    ids_ref[...] = jnp.broadcast_to(
        rows.astype(I32)[:, None, :], (device_count, 8, LANES)
    )

    thermal32[...] = thermal_ref[...].astype(F32)
    kinetic32[...] = kinetic_ref[...].astype(F32)
    part_ref[...] = jnp.zeros_like(part_ref)
    within = iota((WINDOW, BLOCK), 0)

    def add_window(i, base):
        def pair(ref):
            return jnp.concatenate([ref[pl.ds(2 * i, 1), :], ref[pl.ds(2 * i + 1, 1), :]], axis=1)

        base = pl.multiple_of(base, 8)
        match = within + base == pair(slot_ref)
        weights = jnp.concatenate(
            [jnp.where(match, pair(thermal32), 0.0), jnp.where(match, pair(kinetic32), 0.0)], axis=0
        ).astype(BF16)
        sums = dot(weights, kern_ref[pl.ds(pl.multiple_of(i * BLOCK, BLOCK), BLOCK), :])
        part_ref[pl.ds(base, WINDOW), 0:LANES] += sums[:WINDOW]
        part_ref[pl.ds(base, WINDOW), LANES:2 * LANES] += sums[WINDOW:]

    per = blocks // pieces
    for q in range(pieces):
        fetch(q).wait()

        def first_window(i, unused):
            add_window(i, base_ref[i])
            return unused

        lax.fori_loop(q * per, (q + 1) * per, first_window, 0, unroll=4)

    def more_windows(i, unused):
        base = base_ref[i]
        extra = (last_ref[i] - base) // WINDOW

        def one(w, unused):
            add_window(i, base + w * WINDOW)
            return unused

        return lax.fori_loop(1, extra + 1, one, unused)

    lax.fori_loop(0, blocks, more_windows, 0)

    split_ref[...] = halves(part_ref[0:slots, :])
    some = min(256, device_count * cap)

    def permute(i, unused):
        start = pl.multiple_of(i * some, some)
        moved = dot(onehot(iota((some, slots), 0) + start == bucket), split_ref[...])
        out_ref[pl.ds(start, some), :] = moved[:, :2 * LANES] + moved[:, 2 * LANES:]
        return unused

    lax.fori_loop(0, device_count * cap // some, permute, 0)


def exchange(
    dims, out_hbm, ids_hbm, code_ref, owned_ref, shell_ref, arrived, ids, gathered,
    send_sem, recv_sem, ids_send, ids_recv, local_sem, own_send, own_recv, far_send, far_recv,
    pass_send, pass_recv,
):
    vol_count, pix_count, slots, block_tiles, owned_most, cap = dims
    device_count = vol_count * pix_count
    vol, pix = lax.axis_index("vol"), lax.axis_index("pix")
    me = vol * pix_count + pix
    width = 2 * LANES

    def peer(k):
        other_vol = (vol + k // pix_count) % vol_count
        other_pix = (pix + k % pix_count) % pix_count
        return other_vol, other_pix

    barrier = pltpu.get_barrier_semaphore()

    def greet(k, unused):
        pl.semaphore_signal(barrier, inc=1, device_id=peer(k), device_id_type=MESH)
        return unused

    lax.fori_loop(1, device_count, greet, 0)
    pl.semaphore_wait(barrier, device_count - 1)

    def ids_copy(k):
        other_vol, other_pix = peer(k)
        return pltpu.make_async_remote_copy(
            src_ref=ids_hbm.at[other_vol * pix_count + other_pix], dst_ref=ids.at[me],
            send_sem=ids_send.at[k], recv_sem=ids_recv.at[k],
            device_id=(other_vol, other_pix), device_id_type=MESH,
        )

    def rows_copy(k):
        other_vol, other_pix = peer(k)
        return pltpu.make_async_remote_copy(
            src_ref=out_hbm.at[pl.ds((other_vol * pix_count + other_pix) * cap, cap)],
            dst_ref=arrived.at[pl.ds(me * cap, cap)],
            send_sem=send_sem.at[k], recv_sem=recv_sem.at[k],
            device_id=(other_vol, other_pix), device_id_type=MESH,
        )

    def send(k, unused):
        ids_copy(k).start()
        rows_copy(k).start()
        return unused

    lax.fori_loop(1, device_count, send, 0)
    local_ids = pltpu.make_async_copy(ids_hbm.at[me], ids.at[me], local_sem.at[0])
    local_rows = pltpu.make_async_copy(
        out_hbm.at[pl.ds(me * cap, cap)], arrived.at[pl.ds(me * cap, cap)], local_sem.at[1]
    )
    local_ids.start()
    local_rows.start()
    local_ids.wait()
    local_rows.wait()

    group = pix_count * cap
    share = LANES // cap
    own = gathered.at[pix]
    own[...] = jnp.zeros((owned_most, width), F32)
    lane_part = iota((1, LANES), 1) // cap

    def receive(i, unused):
        def one(j, unused):
            k = i * pix_count + j
            ids_copy(k).wait_recv()
            rows_copy(k).wait_recv()
            return unused

        lax.fori_loop(jnp.where(i == 0, 1, 0), pix_count, one, 0)
        sender = (vol + vol_count - i) % vol_count
        pieces = []
        for tau in range(group // LANES):
            piece = jnp.full((1, LANES), -1, I32)
            for g in range(share):
                line = ids[sender * pix_count + tau * share + g]
                piece = jnp.where(lane_part == g, line[0:1], piece)
            pieces.append(piece)
        rows = jnp.concatenate(pieces, axis=1) if len(pieces) > 1 else pieces[0]
        places = onehot(iota((owned_most, group), 0) == rows)
        start = pl.multiple_of(sender * group, group)
        moved = dot(places, halves(arrived[pl.ds(start, group), :]))
        own[...] += moved[:, :width] + moved[:, width:]
        return unused

    lax.fori_loop(0, vol_count, receive, 0)

    core = pix % 2
    sibling = (vol, pix - core + (1 - core))
    far_count = pix_count // 2 - 1
    quarter_count = far_send.shape[1]
    quarter = owned_most // quarter_count

    def far_copy(k, q):
        to = (pix + 2 * k) % pix_count
        rows = pl.ds(q * quarter, quarter)
        return pltpu.make_async_remote_copy(
            src_ref=gathered.at[pix, rows], dst_ref=gathered.at[pix, rows],
            send_sem=far_send.at[k, q], recv_sem=far_recv.at[k, q],
            device_id=(vol, to), device_id_type=MESH,
        )

    def pass_copy(k, q):
        source = (pix + pix_count - 2 * k) % pix_count
        rows = pl.ds(q * quarter, quarter)
        return pltpu.make_async_remote_copy(
            src_ref=gathered.at[source, rows], dst_ref=gathered.at[source, rows],
            send_sem=pass_send.at[k, q], recv_sem=pass_recv.at[k, q],
            device_id=sibling, device_id_type=MESH,
        )

    own_copy = pltpu.make_async_remote_copy(
        src_ref=gathered.at[pix], dst_ref=gathered.at[pix],
        send_sem=own_send.at[0], recv_sem=own_recv.at[0],
        device_id=sibling, device_id_type=MESH,
    )
    for q in range(quarter_count):
        for k in range(1, far_count + 1):
            far_copy(k, q).start()
    own_copy.start()
    owned_ref[...] = own[...]

    def gather(p, start):
        data = halves(gathered[p])

        def one(h, unused):
            at = pl.ds(pl.multiple_of(h * LANES, LANES), LANES)
            codes = code_ref[at, :] - p * owned_most
            places = jnp.concatenate(
                [
                    onehot(codes == iota((LANES, LANES), 1) + r * LANES)
                    for r in range(owned_most // LANES)
                ],
                axis=1,
            )
            moved = dot(places, data)
            moved = moved[:, :width] + moved[:, width:]
            if start:
                shell_ref[at, :] = moved
            else:
                shell_ref[at, :] += moved
            return unused

        lax.fori_loop(0, block_tiles // LANES, one, 0)

    gather(pix, True)
    for q in range(quarter_count):
        for k in range(1, far_count + 1):
            far_copy(k, q).wait_recv()
            pass_copy(k, q).start()
    own_copy.wait_recv()
    gather(sibling[1], False)
    for k in range(1, far_count + 1):
        gather((pix + pix_count - 2 * k) % pix_count, False)
        for q in range(quarter_count):
            pass_copy(k, q).wait_recv()
        gather((sibling[1] + pix_count - 2 * k) % pix_count, False)

    own_copy.wait_send()
    for q in range(quarter_count):
        for k in range(1, far_count + 1):
            far_copy(k, q).wait_send()
            pass_copy(k, q).wait_send()

    def sent(k, unused):
        ids_copy(k).wait_send()
        rows_copy(k).wait_send()
        return unused

    lax.fori_loop(1, device_count, sent, 0)


def shards(kernel, pressure, velocity, entry_slot, slot_tile, tile_owner):
    vol_count, pix_count = lax.axis_size("vol"), lax.axis_size("pix")
    device_count = vol_count * pix_count
    entries = kernel.shape[0]
    slots = slot_tile.shape[1]
    tiles = tile_owner.shape[0]
    block_tiles = tiles // vol_count
    owned_most = 2 * block_tiles // pix_count
    cap = 2 * slots // device_count
    width = 2 * kernel.shape[1]
    dims = (vol_count, pix_count, slots, block_tiles, owned_most, cap)
    vmem = pl.BlockSpec(memory_space=pltpu.VMEM)
    smem = pl.BlockSpec(memory_space=pltpu.SMEM)
    anywhere = pl.BlockSpec(memory_space=pl.ANY)
    dma = pltpu.SemaphoreType.DMA

    ends = entry_slot.reshape(entries // BLOCK, BLOCK)
    base = ends[:, 0] // 8 * 8
    last = ends[:, BLOCK - 1]
    shape = (entries // LANES, LANES)
    outgoing, ids, codes = pl.pallas_call(
        functools.partial(prepare, dims),
        out_shape=(
            jax.ShapeDtypeStruct((device_count * cap, width), F32),
            jax.ShapeDtypeStruct((device_count, 8, LANES), I32),
            jax.ShapeDtypeStruct((block_tiles, LANES), I32),
        ),
        in_specs=[smem, smem, anywhere, vmem, vmem, vmem, vmem, vmem],
        out_specs=(vmem, vmem, vmem),
        scratch_shapes=[
            pltpu.VMEM(kernel.shape, BF16),
            pltpu.VMEM(shape, F32),
            pltpu.VMEM(shape, F32),
            pltpu.VMEM((slots + WINDOW, width), F32),
            pltpu.VMEM((slots, 2 * width), BF16),
            dma((4,)),
        ],
        name="prepare",
    )(
        base, last, kernel, pressure.reshape(shape), velocity.reshape(shape),
        entry_slot.reshape(shape), slot_tile, tile_owner.reshape(tiles // LANES, LANES),
    )

    quarters = 4
    chips = pix_count // 2
    return pl.pallas_call(
        functools.partial(exchange, dims),
        out_shape=(
            jax.ShapeDtypeStruct((owned_most, width), F32),
            jax.ShapeDtypeStruct((block_tiles, width), F32),
        ),
        in_specs=[anywhere, anywhere, vmem],
        out_specs=(vmem, vmem),
        scratch_shapes=[
            pltpu.VMEM((device_count * cap, width), F32),
            pltpu.VMEM((device_count, 8, LANES), I32),
            pltpu.VMEM((pix_count, owned_most, width), F32),
            dma((device_count,)), dma((device_count,)), dma((device_count,)), dma((device_count,)),
            dma((2,)), dma((1,)), dma((1,)),
            dma((chips, quarters)), dma((chips, quarters)),
            dma((chips, quarters)), dma((chips, quarters)),
        ],
        compiler_params=pltpu.CompilerParams(collective_id=0, has_side_effects=True),
        name="exchange",
    )(outgoing, ids, codes)


def solution(mesh):
    in_specs = (
        P(("vol", "pix"), None),
        P(("vol", "pix")),
        P(("vol", "pix")),
        P(("vol", "pix"), None),
        P(("vol", "pix"), None),
        P(),
    )
    out_specs = (P(("vol", "pix"), None), P("vol", None))
    return jax.shard_map(shards, mesh=mesh, in_specs=in_specs, out_specs=out_specs, check_vma=False)
```

```python
import functools

import jax
import jax.numpy as jnp
from jax import lax
from jax.experimental import pallas as pl
from jax.experimental.pallas import tpu as pltpu
from jax.sharding import PartitionSpec as P

MESH = pl.DeviceIdType.MESH
LANES = 128
BLOCK = 256
WINDOW = 48
F32 = jnp.float32
BF16 = jnp.bfloat16
I32 = jnp.int32


def iota(shape, axis):
    return lax.broadcasted_iota(I32, shape, axis)


def onehot(mask):
    return jnp.where(mask, 1.0, 0.0).astype(BF16)


def dot(a, b):
    return jnp.dot(a, b, preferred_element_type=F32)


def halves(x):
    high = x.astype(BF16)
    low = (x - high.astype(F32)).astype(BF16)
    return jnp.concatenate([high, low], axis=1)


def prepare(
    dims, base_ref, last_ref, kern_hbm, thermal_ref, kinetic_ref, slot_ref, tile_ref, owner_ref,
    out_ref, ids_ref, code_ref, kern_ref, thermal32, kinetic32, part_ref, split_ref, all_codes,
    sems,
):
    vol_count, pix_count, slots, block_tiles, owned_most, cap = dims
    device_count = vol_count * pix_count
    entries = kern_ref.shape[0]
    blocks = entries // BLOCK
    pieces = sems.shape[0]
    piece = entries // pieces

    def fetch(q):
        rows = pl.ds(q * piece, piece)
        return pltpu.make_async_copy(kern_hbm.at[rows], kern_ref.at[rows], sems.at[q])

    for q in range(pieces):
        fetch(q).start()

    high_count = owner_ref.shape[0]
    block_high = block_tiles // LANES
    owner = jnp.transpose(owner_ref[...].astype(F32))
    lower = onehot(iota((LANES, LANES), 1) < iota((LANES, LANES), 0))
    first, second = iota((high_count, high_count), 0), iota((high_count, high_count), 1)
    before = onehot((first < second) & (first // block_high == second // block_high))
    rank = jnp.zeros((LANES, high_count), F32)
    for p in range(pix_count):
        mine = owner == p
        ones = jnp.where(mine, 1.0, 0.0)
        inside = dot(lower, ones.astype(BF16))
        total = jnp.broadcast_to(jnp.sum(ones, axis=0, keepdims=True), (8, high_count))
        ahead = dot(total.astype(BF16), before)[0:1]
        rank = rank + jnp.where(mine, inside + ahead, 0.0)

    all_codes[...] = jnp.transpose(owner * owned_most + rank).astype(I32)
    first_high = pl.multiple_of(lax.axis_index("vol") * block_high, block_high)
    code_ref[...] = all_codes[pl.ds(first_high, block_high), :]

    parts = max(1, owned_most // 256)
    rank_high = jnp.floor(rank * (1.0 / 256.0))
    rank_low = rank - 256.0 * rank_high
    table = jnp.concatenate([owner * parts + rank_high, rank_low], axis=0).astype(BF16)
    tile = tile_ref[...]
    high, low = tile // LANES, tile % LANES
    found = dot(table, onehot(iota((high_count, slots), 0) == high))
    pick = iota((LANES, slots), 0) == low
    both = jnp.sum(jnp.where(pick, found[:LANES], 0.0), axis=0, keepdims=True).astype(I32)
    row_low = jnp.sum(jnp.where(pick, found[LANES:], 0.0), axis=0, keepdims=True)
    slot_owner = both // parts
    row_high = (both - slot_owner * parts).astype(F32)
    target = high // block_high * pix_count + slot_owner
    to_device = iota((device_count, slots), 0) == target
    ones = jnp.where(to_device, 1.0, 0.0)
    upper = onehot(iota((LANES, LANES), 0) < iota((LANES, LANES), 1))
    carry = jnp.zeros((device_count, 1), F32)
    position = []
    for j in range(slots // LANES):
        chunk = ones[:, j * LANES:(j + 1) * LANES]
        ranks = dot(chunk.astype(BF16), upper) + carry
        position.append(jnp.sum(chunk * ranks, axis=0, keepdims=True))
        carry = carry + jnp.sum(chunk, axis=1, keepdims=True)
    position = jnp.concatenate(position, axis=1).astype(I32)
    bucket = target * cap + position

    places = onehot(iota((LANES, slots), 0) % cap == position)
    values = jnp.concatenate(
        [jnp.where(to_device, row_high, 0.0), jnp.where(to_device, row_low + 1.0, 0.0)], axis=0
    )
    placed = lax.dot_general(
        values.astype(BF16), places, (((1,), (1,)), ((), ())), preferred_element_type=F32
    )
    rows = placed[:device_count] * 256.0 + placed[device_count:] - 1.0
    ids_ref[...] = jnp.broadcast_to(
        rows.astype(I32)[:, None, :], (device_count, 8, LANES)
    )

    thermal32[...] = thermal_ref[...].astype(F32)
    kinetic32[...] = kinetic_ref[...].astype(F32)
    part_ref[...] = jnp.zeros_like(part_ref)
    within = iota((WINDOW, BLOCK), 0)

    def add_window(i, base):
        def pair(ref):
            return jnp.concatenate([ref[pl.ds(2 * i, 1), :], ref[pl.ds(2 * i + 1, 1), :]], axis=1)

        base = pl.multiple_of(base, 8)
        match = within + base == pair(slot_ref)
        weights = jnp.concatenate(
            [jnp.where(match, pair(thermal32), 0.0), jnp.where(match, pair(kinetic32), 0.0)], axis=0
        ).astype(BF16)
        sums = dot(weights, kern_ref[pl.ds(pl.multiple_of(i * BLOCK, BLOCK), BLOCK), :])
        part_ref[pl.ds(base, WINDOW), 0:LANES] += sums[:WINDOW]
        part_ref[pl.ds(base, WINDOW), LANES:2 * LANES] += sums[WINDOW:]

    per = blocks // pieces
    for q in range(pieces):
        fetch(q).wait()

        def first_window(i, unused):
            add_window(i, base_ref[i])
            return unused

        lax.fori_loop(q * per, (q + 1) * per, first_window, 0, unroll=4)

    def more_windows(i, unused):
        base = base_ref[i]
        extra = (last_ref[i] - base) // WINDOW

        def one(w, unused):
            add_window(i, base + w * WINDOW)
            return unused

        return lax.fori_loop(1, extra + 1, one, unused)

    lax.fori_loop(0, blocks, more_windows, 0)

    split_ref[...] = halves(part_ref[0:slots, :])
    some = min(256, device_count * cap)

    def permute(i, unused):
        start = pl.multiple_of(i * some, some)
        moved = dot(onehot(iota((some, slots), 0) + start == bucket), split_ref[...])
        out_ref[pl.ds(start, some), :] = moved[:, :2 * LANES] + moved[:, 2 * LANES:]
        return unused

    lax.fori_loop(0, device_count * cap // some, permute, 0)


def exchange(
    dims, out_hbm, ids_hbm, code_ref, owned_ref, shell_ref, arrived, ids, sums, crossed, gathered,
    send_sem, recv_sem, ids_send, ids_recv, local_sem, mid_send, mid_recv, own_send, own_recv,
    far_send, far_recv, pass_send, pass_recv,
):
    vol_count, pix_count, slots, block_tiles, owned_most, cap = dims
    half = vol_count // 2
    near_count = half * pix_count
    vol, pix = lax.axis_index("vol"), lax.axis_index("pix")
    side, place = vol // half, vol % half
    mine = place * pix_count + pix
    across = (vol + half) % vol_count
    width = 2 * LANES

    def peer(k):
        return side * half + (place + k // pix_count) % half, (pix + k % pix_count) % pix_count

    barrier = pltpu.get_barrier_semaphore()

    def greet(k, unused):
        pl.semaphore_signal(barrier, inc=1, device_id=peer(k), device_id_type=MESH)
        return unused

    pl.semaphore_signal(barrier, inc=1, device_id=(across, pix), device_id_type=MESH)
    lax.fori_loop(1, near_count, greet, 0)
    pl.semaphore_wait(barrier, near_count)

    def final(stage, other_vol, other_pix):
        return (other_vol + half * (1 - stage)) % vol_count * pix_count + other_pix

    def ids_copy(stage, k):
        other_vol, other_pix = peer(k)
        return pltpu.make_async_remote_copy(
            src_ref=ids_hbm.at[final(stage, other_vol, other_pix)], dst_ref=ids.at[stage, mine],
            send_sem=ids_send.at[stage, k], recv_sem=ids_recv.at[stage, k],
            device_id=(other_vol, other_pix), device_id_type=MESH,
        )

    def rows_copy(stage, k):
        other_vol, other_pix = peer(k)
        return pltpu.make_async_remote_copy(
            src_ref=out_hbm.at[pl.ds(final(stage, other_vol, other_pix) * cap, cap)],
            dst_ref=arrived.at[stage, pl.ds(mine * cap, cap)],
            send_sem=send_sem.at[stage, k], recv_sem=recv_sem.at[stage, k],
            device_id=(other_vol, other_pix), device_id_type=MESH,
        )

    def local_copies(stage):
        own = final(stage, vol, pix)
        return (
            pltpu.make_async_copy(ids_hbm.at[own], ids.at[stage, mine], local_sem.at[stage, 0]),
            pltpu.make_async_copy(
                out_hbm.at[pl.ds(own * cap, cap)], arrived.at[stage, pl.ds(mine * cap, cap)],
                local_sem.at[stage, 1],
            ),
        )

    for stage in range(2):

        def send(k, unused):
            ids_copy(stage, k).start()
            rows_copy(stage, k).start()
            return unused

        for copy in local_copies(stage):
            copy.start()
        lax.fori_loop(1, near_count, send, 0)

    group = pix_count * cap
    share = LANES // cap
    lane_part = iota((1, LANES), 1) // cap

    def sum_up(stage, target):
        for copy in local_copies(stage):
            copy.wait()
        target[...] = jnp.zeros((owned_most, width), F32)

        def receive(i, unused):
            def one(j, unused):
                k = i * pix_count + j
                ids_copy(stage, k).wait_recv()
                rows_copy(stage, k).wait_recv()
                return unused

            lax.fori_loop(jnp.where(i == 0, 1, 0), pix_count, one, 0)
            sender = (place + half - i) % half
            pieces = []
            for tau in range(group // LANES):
                piece = jnp.full((1, LANES), -1, I32)
                for g in range(share):
                    line = ids[stage, sender * pix_count + tau * share + g]
                    piece = jnp.where(lane_part == g, line[0:1], piece)
                pieces.append(piece)
            rows = jnp.concatenate(pieces, axis=1) if len(pieces) > 1 else pieces[0]
            places = onehot(iota((owned_most, group), 0) == rows)
            start = pl.multiple_of(sender * group, group)
            moved = dot(places, halves(arrived[stage, pl.ds(start, group), :]))
            target[...] += moved[:, :width] + moved[:, width:]
            return unused

        lax.fori_loop(0, half, receive, 0)

    piece_count = mid_send.shape[0]
    piece_rows = owned_most // piece_count

    def part(q):
        return pl.ds(q * piece_rows, piece_rows)

    def mid_copy(q):
        return pltpu.make_async_remote_copy(
            src_ref=sums.at[part(q)], dst_ref=crossed.at[part(q)],
            send_sem=mid_send.at[q], recv_sem=mid_recv.at[q],
            device_id=(across, pix), device_id_type=MESH,
        )

    sum_up(0, sums)
    for q in range(piece_count):
        mid_copy(q).start()
    own = gathered.at[pix]
    sum_up(1, own)

    core = pix % 2
    sibling = (vol, pix - core + (1 - core))
    others = range(1, pix_count // 2)

    def far_copy(k, q):
        return pltpu.make_async_remote_copy(
            src_ref=gathered.at[pix, part(q)], dst_ref=gathered.at[pix, part(q)],
            send_sem=far_send.at[k, q], recv_sem=far_recv.at[k, q],
            device_id=(vol, (pix + 2 * k) % pix_count), device_id_type=MESH,
        )

    def pass_copy(k, q):
        source = (pix + pix_count - 2 * k) % pix_count
        return pltpu.make_async_remote_copy(
            src_ref=gathered.at[source, part(q)], dst_ref=gathered.at[source, part(q)],
            send_sem=pass_send.at[k, q], recv_sem=pass_recv.at[k, q],
            device_id=sibling, device_id_type=MESH,
        )

    def own_copy(q):
        return pltpu.make_async_remote_copy(
            src_ref=gathered.at[pix, part(q)], dst_ref=gathered.at[pix, part(q)],
            send_sem=own_send.at[q], recv_sem=own_recv.at[q],
            device_id=sibling, device_id_type=MESH,
        )

    def relay(q):
        for k in others:
            far_copy(k, q).wait_recv()
            pass_copy(k, q).start()

    for q in range(piece_count):
        mid_copy(q).wait_recv()
        whole = own[part(q), :] + crossed[part(q), :]
        own[part(q), :] = whole
        owned_ref[part(q), :] = whole
        for k in others:
            far_copy(k, q).start()
        own_copy(q).start()
        if q:
            relay(q - 1)
    relay(piece_count - 1)
    for q in range(piece_count):
        own_copy(q).wait()
        mid_copy(q).wait_send()
        for k in others:
            far_copy(k, q).wait_send()
            pass_copy(k, q).wait()

    def gather(i, unused):
        lines = []
        for j in range(8):
            code = code_ref[i * 8 + j]
            source = code // owned_most
            lines.append(gathered[source, pl.ds(code - source * owned_most, 1), :])
        shell_ref[pl.ds(pl.multiple_of(i * 8, 8), 8), :] = jnp.concatenate(lines, axis=0)
        return unused

    lax.fori_loop(0, block_tiles // 8, gather, 0, unroll=2)

    for stage in range(2):

        def sent(k, unused):
            ids_copy(stage, k).wait_send()
            rows_copy(stage, k).wait_send()
            return unused

        lax.fori_loop(1, near_count, sent, 0)


def shards(kernel, pressure, velocity, entry_slot, slot_tile, tile_owner):
    vol_count, pix_count = lax.axis_size("vol"), lax.axis_size("pix")
    device_count = vol_count * pix_count
    entries = kernel.shape[0]
    slots = slot_tile.shape[1]
    tiles = tile_owner.shape[0]
    block_tiles = tiles // vol_count
    owned_most = 2 * block_tiles // pix_count
    cap = 2 * slots // device_count
    width = 2 * kernel.shape[1]
    dims = (vol_count, pix_count, slots, block_tiles, owned_most, cap)
    vmem = pl.BlockSpec(memory_space=pltpu.VMEM)
    smem = pl.BlockSpec(memory_space=pltpu.SMEM)
    anywhere = pl.BlockSpec(memory_space=pl.ANY)
    dma = pltpu.SemaphoreType.DMA

    ends = entry_slot.reshape(entries // BLOCK, BLOCK)
    base = ends[:, 0] // 8 * 8
    last = ends[:, BLOCK - 1]
    shape = (entries // LANES, LANES)
    outgoing, ids, codes = pl.pallas_call(
        functools.partial(prepare, dims),
        out_shape=(
            jax.ShapeDtypeStruct((device_count * cap, width), F32),
            jax.ShapeDtypeStruct((device_count, 8, LANES), I32),
            jax.ShapeDtypeStruct((block_tiles // LANES, LANES), I32),
        ),
        in_specs=[smem, smem, anywhere, vmem, vmem, vmem, vmem, vmem],
        out_specs=(vmem, vmem, vmem),
        scratch_shapes=[
            pltpu.VMEM(kernel.shape, BF16),
            pltpu.VMEM(shape, F32),
            pltpu.VMEM(shape, F32),
            pltpu.VMEM((slots + WINDOW, width), F32),
            pltpu.VMEM((slots, 2 * width), BF16),
            pltpu.VMEM((tiles // LANES, LANES), I32),
            dma((4,)),
        ],
        name="prepare",
    )(
        base, last, kernel, pressure.reshape(shape), velocity.reshape(shape),
        entry_slot.reshape(shape), slot_tile, tile_owner.reshape(tiles // LANES, LANES),
    )

    pieces = 4
    chips = pix_count // 2
    near = device_count // 2
    return pl.pallas_call(
        functools.partial(exchange, dims),
        out_shape=(
            jax.ShapeDtypeStruct((owned_most, width), F32),
            jax.ShapeDtypeStruct((block_tiles, width), F32),
        ),
        in_specs=[anywhere, anywhere, smem],
        out_specs=(vmem, vmem),
        scratch_shapes=[
            pltpu.VMEM((2, near * cap, width), F32),
            pltpu.VMEM((2, near, 8, LANES), I32),
            pltpu.VMEM((owned_most, width), F32),
            pltpu.VMEM((owned_most, width), F32),
            pltpu.VMEM((pix_count, owned_most, width), F32),
            dma((2, near)), dma((2, near)), dma((2, near)), dma((2, near)),
            dma((2, 2)), dma((pieces,)), dma((pieces,)), dma((pieces,)), dma((pieces,)),
            dma((chips, pieces)), dma((chips, pieces)), dma((chips, pieces)), dma((chips, pieces)),
        ],
        compiler_params=pltpu.CompilerParams(collective_id=0, has_side_effects=True),
        name="exchange",
    )(outgoing, ids, codes.reshape(block_tiles))


def solution(mesh):
    in_specs = (
        P(("vol", "pix"), None),
        P(("vol", "pix")),
        P(("vol", "pix")),
        P(("vol", "pix"), None),
        P(("vol", "pix"), None),
        P(),
    )
    out_specs = (P(("vol", "pix"), None), P("vol", None))
    return jax.shard_map(shards, mesh=mesh, in_specs=in_specs, out_specs=out_specs, check_vma=False)
```
